256 devices in a mesh: band: 32 (over z, x_hi, core), dom: 8 (over x_lo, y).
Axes of the slice: x: 4 (x_hi: 2, x_lo: 2; x = x_hi * 2 + x_lo), y: 4, z: 8, core: 2. Of those that a mesh axis runs over, the one named last changes fastest.
Arguments:
- orbitals: bfloat16 [256, 128, 128, 128], P('band', None, 'dom'), may hold values from -6 to 6
- occupations: float32 [256], P('band'), may hold values from 0.25 to 2
Outputs:
- potential: float32 [256, 256, 256], P('band', 'dom')
The draws below stay inside these ranges and needn't reach their ends.
All inputs are finite; a program needn't handle non-finite values.
Results may differ from the reference program's by a relative error of at most 0.0003.
Values sent between devices are 32-bit elements; how exact they have to be, the bound alone decides.
A program may use at most 64 MiB of HBM per device.

```python
import math
import jax
import jax.numpy as jnp
from jax import lax

N3 = 128
BANDS = 256
N1 = 128
N2 = 128


def raised(result, rng, source, target, shards_of, factor):
    def block_of(dim):
        return (jnp.arange(result.shape[dim]) // (result.shape[dim] // shards_of)).reshape((-1,) + (1,) * (result.ndim - 1 - dim))

    near = jax.random.permutation(rng, shards_of)[block_of(target)]
    second = (block_of(target) + shards_of // 2) % shards_of
    return jnp.where((block_of(source) == near) | (block_of(source) == second), factor * result, result)


def steps_of(stream_key, shape, pieces, low, top_value):
    level, own = 1.0, jax.random.fold_in(stream_key, 6)
    for axis_at, shards_of in pieces:
        draws = jnp.exp(jax.random.uniform(jax.random.fold_in(own, axis_at), (shards_of,), jnp.float32, low / len(pieces), top_value / len(pieces)))
        level = level * jnp.repeat(draws, shape[axis_at] // shards_of).reshape([-1 if axis == axis_at else 1 for axis in range(len(shape))])
    return level


def heavy_noise(rng, dims, scale, reach, shards, heavy, kind=jnp.bfloat16):
    values = scale * jax.random.normal(rng, dims, jnp.float32)
    if shards:
        values = values * steps_of(rng, dims, shards, -0.22, 0.18)
    return jnp.clip(raised(values, jax.random.fold_in(rng, 3), *heavy), -reach, reach).astype(kind)


def setup_inputs(seed: int = 0) -> dict:
    splits = jax.random.split(jax.random.key(seed), 3)
    orbitals = heavy_noise(splits[0], (BANDS, N1, N2, N3), 1.0, 6.0, ((0, 32), (2, 8)), (0, 1, 32, 2.75))
    occupations = jnp.clip(jnp.exp(math.log(2.0) - 2.0794415 * jax.random.uniform(splits[1], (BANDS,), jnp.float32) ** steps_of(splits[1], (BANDS,), ((0, 32),), -0.2, 0.2)), 0.25, 2.0)
    return dict(orbitals=orbitals, occupations=occupations)


interp_weights = (3.0 / 256.0, -25.0 / 256.0, 150.0 / 256.0, 150.0 / 256.0, -25.0 / 256.0, 3.0 / 256.0)
deriv_factors = (4.0 / 5.0, -1.0 / 5.0, 4.0 / 105.0, -1.0 / 280.0)


def alternate(even_cells, odd_cells, along):
    stacked = jnp.stack([even_cells, odd_cells], axis=along + 1)
    target_shape = list(even_cells.shape)
    target_shape[along] = 2 * even_cells.shape[along]
    return stacked.reshape(target_shape)


def refine(padded, along, extent):
    odd_cells = jnp.zeros_like(lax.slice_in_dim(padded, 3, 3 + extent, axis=along))
    for offset, factor in zip(range(-2, 4), interp_weights):
        odd_cells = odd_cells + factor * lax.slice_in_dim(padded, 3 + offset, 3 + offset + extent, axis=along)
    even_cells = lax.slice_in_dim(padded, 3, 3 + extent, axis=along)
    return alternate(even_cells, odd_cells, along)


def central(padded, along, start_a, start_b, extent_a, extent_b):
    window_base = padded[start_a:start_a + extent_a, start_b:start_b + extent_b]
    summed = jnp.zeros_like(window_base)
    for offset, factor in zip((1, 2, 3, 4), deriv_factors):
        if along == 0:
            ahead_part = padded[start_a + offset:start_a + offset + extent_a, start_b:start_b + extent_b]
            behind_part = padded[start_a - offset:start_a - offset + extent_a, start_b:start_b + extent_b]
        elif along == 1:
            ahead_part = padded[start_a:start_a + extent_a, start_b + offset:start_b + offset + extent_b]
            behind_part = padded[start_a:start_a + extent_a, start_b - offset:start_b - offset + extent_b]
        else:
            ahead_part = jnp.roll(window_base, -offset, 2)
            behind_part = jnp.roll(window_base, offset, 2)
        summed = summed + factor * (ahead_part - behind_part)
    return summed


def pointwise(density, grad_a, grad_b, grad_c):
    shifted = density * density + 0.01
    scaling = 0.01 * shifted ** (4.0 / 3.0)
    reduced = (grad_a * grad_a + grad_b * grad_b + grad_c * grad_c) / scaling
    divisor = 1.0 + 0.2195 * reduced / 0.804
    enhance = 0.804 - 0.804 / divisor
    flux_weight = 0.2195 / (divisor * divisor) / scaling
    local_part = -0.75 * shifted ** (1.0 / 6.0) * (1.0 + enhance)
    return local_part, flux_weight * grad_a, flux_weight * grad_b, flux_weight * grad_c


def reference(orbitals, occupations):
    weights = occupations / orbitals.shape[0]

    def add_band(index, summed):
        return summed + weights[index] * jnp.square(orbitals[index].astype(jnp.float32))

    density = lax.fori_loop(0, orbitals.shape[0], add_band, jnp.zeros(orbitals.shape[1:], jnp.float32))
    fine = density
    for along in (0, 1, 2):
        widths = [(0, 0), (0, 0), (0, 0)]
        widths[along] = (3, 3)
        fine = refine(jnp.pad(fine, widths, mode="wrap"), along, fine.shape[along])
    extent_a, extent_b = fine.shape[0], fine.shape[1]
    padded = jnp.pad(fine, ((4, 4), (4, 4), (0, 0)), mode="wrap")
    grad_a = central(padded, 0, 4, 4, extent_a, extent_b)
    grad_b = central(padded, 1, 4, 4, extent_a, extent_b)
    grad_c = central(padded, 2, 4, 4, extent_a, extent_b)
    local_part, flux_a, flux_b, flux_c = pointwise(fine, grad_a, grad_b, grad_c)
    div_a = central(jnp.pad(flux_a, ((4, 4), (0, 0), (0, 0)), mode="wrap"), 0, 4, 0, extent_a, extent_b)
    div_b = central(jnp.pad(flux_b, ((0, 0), (4, 4), (0, 0)), mode="wrap"), 1, 0, 4, extent_a, extent_b)
    div_c = central(flux_c, 2, 0, 0, extent_a, extent_b)
    return local_part + 0.2 * (div_a + div_b + div_c)
```

```python
import jax
import jax.numpy as jnp
from jax import lax
from jax.experimental import pallas as pl
from jax.experimental.pallas import tpu as pltpu
from jax.sharding import PartitionSpec as P

MESH = pl.DeviceIdType.MESH
W3, W25, W150 = 3.0 / 256.0, -25.0 / 256.0, 150.0 / 256.0
C1, C2, C3, C4 = 4.0 / 5.0, -1.0 / 5.0, 4.0 / 105.0, -1.0 / 280.0

STEPS = (4, 3, 5, 2, 6, 1, 7, 0)
PARTNERS = tuple((j, e) for j in (1, -1, 2, -2, 0) for e in (1, -1, 0) if (j, e) != (0, 0))


def gather_kernel(occ_ref, orb_ref, dens_ref, orb, part, from_core, from_x, from_z,
                  in_sem, core_s, core_r, x_s, x_r, z_s, z_r, halo_s, halo_r):
    band = lax.axis_index("band")
    dom = lax.axis_index("dom")
    z, h, c = band // 4, (band // 2) % 2, band % 2
    other_c, other_h = 1 - c, 1 - h
    core_peer = z * 4 + h * 2 + other_c
    x_peer = z * 4 + other_h * 2 + c

    def z_peer(k):
        return (band + 4 * k) % 32

    def halo_peer(j, e):
        return (band + j + 32) % 32, (dom + e + 8) % 8

    loads = []
    for s, k in enumerate(STEPS):
        first = ((z + k) % 8) * 16
        load = pltpu.make_async_copy(orb_ref.at[:, pl.ds(first, 16)], orb.at[s], in_sem.at[s])
        load.start()
        loads.append(load)

    barrier = pltpu.get_barrier_semaphore()
    peers = [(core_peer, dom), (x_peer, dom)]
    peers += [(z_peer(k), dom) for k in STEPS if k]
    peers += [halo_peer(j, e) for j, e in PARTNERS]
    for b, d in peers:
        pl.semaphore_signal(barrier, inc=1, device_id={"band": b, "dom": d}, device_id_type=MESH)

    weights = [occ_ref[i] * (1.0 / 256.0) for i in range(8)]

    for s in range(8):
        loads[s].wait()

        def planes(block, _):
            for p in range(4):
                total = jnp.zeros((16, 128), jnp.float32)
                for i in range(8):
                    value = orb[s, i, block * 4 + p].astype(jnp.float32)
                    total = total + weights[i] * (value * value)
                part[s, block % 2, block // 2, p] = total
            return 0

        lax.fori_loop(0, 4, planes, 0)

    pl.semaphore_wait(barrier, len(peers))

    to_core = []
    for s in range(8):
        copy = pltpu.make_async_remote_copy(
            src_ref=part.at[s, other_c], dst_ref=from_core.at[s], send_sem=core_s.at[s],
            recv_sem=core_r.at[s], device_id={"band": core_peer, "dom": dom}, device_id_type=MESH)
        copy.start()
        to_core.append(copy)

    to_x = []
    for s in range(8):
        to_core[s].wait_recv()
        from_core[s] = from_core[s] + part[s, c]
        copy = pltpu.make_async_remote_copy(
            src_ref=from_core.at[s, other_h], dst_ref=from_x.at[s], send_sem=x_s.at[s],
            recv_sem=x_r.at[s], device_id={"band": x_peer, "dom": dom}, device_id_type=MESH)
        copy.start()
        to_x.append(copy)

    to_z = []
    for s, k in enumerate(STEPS):
        to_x[s].wait_recv()
        from_x[s] = from_x[s] + from_core[s, h]
        if k:
            copy = pltpu.make_async_remote_copy(
                src_ref=from_x.at[s], dst_ref=from_z.at[s], send_sem=z_s.at[s],
                recv_sem=z_r.at[s], device_id={"band": z_peer(k), "dom": dom}, device_id_type=MESH)
            copy.start()
            to_z.append(copy)

    total = from_x[7]
    for s in range(7):
        to_z[s].wait_recv()
        total = total + from_z[s]
    dens_ref[6:10, 8:24, :] = total

    halos = []
    for n, (j, e) in enumerate(PARTNERS):
        p0, p1, q0 = {0: (0, 4, 6), 1: (0, 4, 2), -1: (0, 4, 10), 2: (2, 4, 0), -2: (0, 3, 14)}[j]
        r0, r1, t0 = {0: (8, 24, 8), 1: (16, 24, 0), -1: (8, 16, 24)}[e]
        b, d = halo_peer(j, e)
        copy = pltpu.make_async_remote_copy(
            src_ref=dens_ref.at[pl.ds(6 + p0, p1 - p0), pl.ds(r0, r1 - r0)],
            dst_ref=dens_ref.at[pl.ds(q0, p1 - p0), pl.ds(t0, r1 - r0)],
            send_sem=halo_s.at[n], recv_sem=halo_r.at[n],
            device_id={"band": b, "dom": d}, device_id_type=MESH)
        copy.start()
        halos.append(copy)
    for copy in to_core + to_x + to_z:
        copy.wait_send()
    for copy in halos:
        copy.wait()


def gathered(orbitals, occupations):
    f32 = jnp.float32
    dma = pltpu.SemaphoreType.DMA
    return pl.pallas_call(
        gather_kernel,
        out_shape=jax.ShapeDtypeStruct((17, 32, 128), f32),
        in_specs=[pl.BlockSpec(memory_space=pltpu.SMEM), pl.BlockSpec(memory_space=pl.ANY)],
        out_specs=pl.BlockSpec(memory_space=pltpu.VMEM),
        scratch_shapes=[
            pltpu.VMEM((8, 8, 16, 16, 128), jnp.bfloat16),
            pltpu.VMEM((8, 2, 2, 4, 16, 128), f32),
            pltpu.VMEM((8, 2, 4, 16, 128), f32),
            pltpu.VMEM((8, 4, 16, 128), f32),
            pltpu.VMEM((7, 4, 16, 128), f32),
            dma((8,)), dma((8,)), dma((8,)), dma((8,)), dma((8,)), dma((7,)), dma((7,)),
            dma((len(PARTNERS),)), dma((len(PARTNERS),)),
        ],
        compiler_params=pltpu.CompilerParams(collective_id=0, has_side_effects=True,
                                             vmem_limit_bytes=67043328),
    )(occupations, orbitals)


def odd_of(v):
    return W3 * (v[0] + v[5]) + W25 * (v[1] + v[4]) + W150 * (v[2] + v[3])


def weighted(d1, d2, d3, d4):
    return C1 * d1 + C2 * d2 + C3 * d3 + C4 * d4


def turned(v, shift):
    return pltpu.roll(v, shift % 128, 1)


def along_lanes(even, odd):
    ep1, em1, ep2, em2 = turned(even, -1), turned(even, 1), turned(even, -2), turned(even, 2)
    op1, om1, op2, om2 = turned(odd, -1), turned(odd, 1), turned(odd, -2), turned(odd, 2)
    at_even = weighted(odd - om1, ep1 - em1, op1 - om2, ep2 - em2)
    at_odd = weighted(ep1 - even, op1 - om1, ep2 - em1, op2 - om2)
    return at_even, at_odd


def across_planes(ref, p, r0, rows):
    def at(o):
        return ref[p + o, pl.ds(r0, rows), :]
    return weighted(*(at(o) - at(-o) for o in (1, 2, 3, 4)))


def across_rows(ref, p, r0, rows):
    def at(o):
        return ref[p, pl.ds(r0 + o, rows), :]
    return weighted(*(at(o) - at(-o) for o in (1, 2, 3, 4)))


def potential_kernel(dens, out, f1, fe, fo, ae, ao, be, bo, ce, co, le, lo):
    def first(i, _):
        v = [dens[i + o] for o in range(6)]
        f1[2 * i] = v[2]
        f1[2 * i + 1] = odd_of(v)
        return 0
    lax.fori_loop(0, 12, first, 0)

    def second(p, _):
        v = [f1[p, pl.ds(2 + o, 24), :] for o in range(6)]
        fe[p, pl.ds(0, 24, stride=2), :] = v[2]
        fe[p, pl.ds(1, 24, stride=2), :] = odd_of(v)
        return 0
    lax.fori_loop(0, 24, second, 0)

    def third(p, _):
        v = fe[p]
        fo[p] = odd_of([turned(v, 2), turned(v, 1), v, turned(v, -1), turned(v, -2), turned(v, -3)])
        return 0
    lax.fori_loop(0, 24, third, 0)

    def flux(p, r0, rows, inner):
        even, odd = fe[p, pl.ds(r0, rows), :], fo[p, pl.ds(r0, rows), :]
        g3e, g3o = along_lanes(even, odd)
        for f, g3, src, a, b, c, local in ((even, g3e, fe, ae, be, ce, le), (odd, g3o, fo, ao, bo, co, lo)):
            g1 = across_planes(src, p, r0, rows)
            g2 = across_rows(src, p, r0, rows)
            shifted = f * f + 0.01
            sixth = jnp.exp(jnp.log(shifted) * (1.0 / 6.0))
            t2 = sixth * sixth
            t4 = t2 * t2
            scaling = 0.01 * (t4 * t4)
            inverse = 1.0 / (scaling + (0.2195 / 0.804) * (g1 * g1 + g2 * g2 + g3 * g3))
            share = scaling * inverse
            weight = (0.2195 * share) * inverse
            a[p - 4, pl.ds(r0, rows), :] = weight * g1
            if inner:
                b[p - 8, pl.ds(r0, rows), :] = weight * g2
                c[p - 8, pl.ds(r0, rows), :] = weight * g3
                local[p - 8, pl.ds(r0, rows), :] = (-0.75 * sixth) * (1.804 - 0.804 * share)

    def outer_low(p, _):
        flux(p, 8, 32, False)
        return 0

    def inner(p, _):
        flux(p, 4, 40, True)
        return 0
    lax.fori_loop(4, 8, outer_low, 0)
    lax.fori_loop(8, 16, inner, 0)
    lax.fori_loop(16, 20, outer_low, 0)

    half = lax.broadcasted_iota(jnp.int32, (32, 128), 1)
    is_even = half % 2 == 0
    low = half // 2
    high = low + 64

    def last(p, _):
        rows = pl.ds(8, 32)
        d3e, d3o = along_lanes(ce[p, rows, :], co[p, rows, :])
        res = []
        for d3, a, b, local in ((d3e, ae, be, le), (d3o, ao, bo, lo)):
            div = across_planes(a, p + 4, 8, 32) + across_rows(b, p, 8, 32) + d3
            res.append(local[p, rows, :] + 0.2 * div)
        for at, lanes in ((0, low), (128, high)):
            e = jnp.take_along_axis(res[0], lanes, axis=1)
            o = jnp.take_along_axis(res[1], lanes, axis=1)
            out[p, :, pl.ds(at, 128)] = jnp.where(is_even, e, o)
        return 0
    lax.fori_loop(0, 8, last, 0)


def potential_of(dens):
    f32 = jnp.float32
    fine = pltpu.VMEM((24, 48, 128), f32)
    wide = pltpu.VMEM((16, 48, 128), f32)
    narrow = pltpu.VMEM((8, 48, 128), f32)
    return pl.pallas_call(
        potential_kernel,
        out_shape=jax.ShapeDtypeStruct((8, 32, 256), f32),
        in_specs=[pl.BlockSpec(memory_space=pltpu.VMEM)],
        out_specs=pl.BlockSpec(memory_space=pltpu.VMEM),
        scratch_shapes=[pltpu.VMEM((24, 32, 128), f32), fine, fine, wide, wide,
                        narrow, narrow, narrow, narrow, narrow, narrow],
        compiler_params=pltpu.CompilerParams(vmem_limit_bytes=40 * 1024 * 1024),
    )(dens)


def on_device(orbitals, occupations):
    return potential_of(gathered(orbitals, occupations))


def solution(mesh):
    return jax.shard_map(
        on_device,
        mesh=mesh,
        in_specs=(P("band", None, "dom", None), P("band")),
        out_specs=P("band", "dom", None),
        check_vma=False,
    )
```

```python
import jax
import jax.numpy as jnp
from jax import lax
from jax.experimental import pallas as pl
from jax.experimental.pallas import tpu as pltpu
from jax.sharding import PartitionSpec as P

MESH = pl.DeviceIdType.MESH
F32, BF16 = jnp.float32, jnp.bfloat16
W3, W25, W150 = 3.0 / 256.0, -25.0 / 256.0, 150.0 / 256.0
REFINE = {-2: W3, -1: W25, 0: W150, 1: W150, 2: W25, 3: W3}
D1, D2, D3, D4 = 224.0, -56.0, 32.0 / 3.0, -1.0
DERIV = {1: D1, 2: D2, 3: D3, 4: D4}

STEPS = (4, 3, 5, 2, 6, 1, 7, 0)
PARTNERS = tuple((j, e) for j in (1, -1, 2, -2, 0) for e in (1, -1, 0) if (j, e) != (0, 0))


def fine_cell(r):
    if r % 2 == 0:
        return {r // 2: 1.0}
    return {(r - 1) // 2 + o: w for o, w in REFINE.items()}


def composed(r):
    out = {}
    for o, c in DERIV.items():
        for sign in (1, -1):
            for m, w in fine_cell(r + sign * o).items():
                out[m] = out.get(m, 0.0) + sign * c * w
    return out


def circulant(factors):
    source = lax.broadcasted_iota(jnp.int32, (128, 128), 0)
    target = lax.broadcasted_iota(jnp.int32, (128, 128), 1)
    offset = (source - target + 128) % 128
    out = jnp.zeros((128, 128), F32)
    for m, w in factors.items():
        out = jnp.where(offset == m % 128, w, out)
    return out


def two_terms(v):
    high = v.astype(BF16)
    return high, (v - high.astype(F32)).astype(BF16)


def build_matrices(wide_w, low_w, deriv_w, weave_w):
    refine = circulant(REFINE).astype(BF16)
    wide_w[0:128, 0:128] = refine
    wide_w[128:256, 0:128] = refine
    for r in (0, 1):
        high, low = two_terms(circulant(composed(r)))
        columns = slice(128 + 128 * r, 256 + 128 * r)
        wide_w[0:128, columns] = high
        wide_w[128:256, columns] = high
        low_w[:, 128 * r:128 * r + 128] = low
    for r in (0, 1):
        source = 2 * lax.broadcasted_iota(jnp.int32, (128, 256), 0) + r
        target = lax.broadcasted_iota(jnp.int32, (128, 256), 1)
        offset = (source - target + 256) % 256
        out = jnp.zeros((128, 256), F32)
        for o, c in ((1, 672.0), (2, -168.0), (3, 32.0), (4, -3.0)):
            out = jnp.where(offset == o, c, jnp.where(offset == 256 - o, -c, out))
        deriv_w[128 * r:128 * r + 128, :] = out.astype(BF16)
        weave_w[128 * r:128 * r + 128, :] = jnp.where(offset == 0, 1.0, 0.0).astype(BF16)


def kernel(occ_hbm, orb_ref, out_ref, occ_ref, occ_sem, dens_ref, orb, part, from_core, from_x, from_z,
           in_sem, core_s, core_r, x_s, x_r, z_s, z_r, halo_s, halo_r, matrices, fields):
    band = lax.axis_index("band")
    dom = lax.axis_index("dom")
    z, h, c = band // 4, (band // 2) % 2, band % 2
    other_c, other_h = 1 - c, 1 - h
    core_peer = z * 4 + h * 2 + other_c
    x_peer = z * 4 + other_h * 2 + c

    def z_peer(k):
        return (band + 4 * k) % 32

    def halo_peer(j, e):
        return (band + j + 32) % 32, (dom + e + 8) % 8

    def remote(src, dst, send_sem, recv_sem, b, d):
        copy = pltpu.make_async_remote_copy(
            src_ref=src, dst_ref=dst, send_sem=send_sem, recv_sem=recv_sem,
            device_id={"band": b, "dom": d}, device_id_type=MESH)
        copy.start()
        return copy

    occ_load = pltpu.make_async_copy(occ_hbm, occ_ref, occ_sem)
    occ_load.start()
    loads = []
    for s, k in enumerate(STEPS):
        first = ((z + k) % 8) * 16
        load = pltpu.make_async_copy(orb_ref.at[:, pl.ds(first, 16)], orb.at[s], in_sem.at[s])
        load.start()
        loads.append(load)

    barrier = pltpu.get_barrier_semaphore()
    peers = [(core_peer, dom), (x_peer, dom)]
    peers += [(z_peer(k), dom) for k in STEPS if k]
    peers += [halo_peer(j, e) for j, e in PARTNERS]
    for b, d in peers:
        pl.semaphore_signal(barrier, inc=1, device_id={"band": b, "dom": d}, device_id_type=MESH)

    occ_load.wait()
    weights = [occ_ref[i] * (1.0 / 256.0) for i in range(8)]

    def band_sum(s):
        loads[s].wait()

        def planes(block, _):
            for p in range(4):
                total = jnp.zeros((16, 128), F32)
                for i in range(8):
                    value = orb[s, i, block * 4 + p].astype(F32)
                    total = total + weights[i] * (value * value)
                part[s, block % 2, block // 2, p] = total
            return 0

        lax.fori_loop(0, 4, planes, 0)

    to_core, to_x, to_z = [], [], []

    def send_core(s):
        to_core.append(remote(part.at[s, other_c], from_core.at[s], core_s.at[s], core_r.at[s],
                              core_peer, dom))

    def send_x(s):
        to_core[s].wait_recv()
        from_core[s] = from_core[s] + part[s, c]
        to_x.append(remote(from_core.at[s, other_h], from_x.at[s], x_s.at[s], x_r.at[s], x_peer, dom))

    for s in range(6):
        band_sum(s)
    pl.semaphore_wait(barrier, len(peers))
    for s in range(6):
        send_core(s)
    band_sum(6)
    send_core(6)
    send_x(0)
    send_x(1)
    band_sum(7)
    send_core(7)
    for s in range(2, 8):
        send_x(s)
    build_matrices(*matrices)
    for s, k in enumerate(STEPS):
        to_x[s].wait_recv()
        from_x[s] = from_x[s] + from_core[s, h]
        if k:
            to_z.append(remote(from_x.at[s], from_z.at[s], z_s.at[s], z_r.at[s], z_peer(k), dom))

    total = from_x[7]
    for s in range(7):
        to_z[s].wait_recv()
        total = total + from_z[s]
    dens_ref[6:10, 8:24, :] = total

    halos = []
    for n, (j, e) in enumerate(PARTNERS):
        p0, p1, q0 = {0: (0, 4, 6), 1: (0, 4, 2), -1: (0, 4, 10), 2: (2, 4, 0), -2: (0, 3, 14)}[j]
        r0, r1, t0 = {0: (8, 24, 8), 1: (16, 24, 0), -1: (8, 16, 24)}[e]
        b, d = halo_peer(j, e)
        halos.append(remote(dens_ref.at[pl.ds(6 + p0, p1 - p0), pl.ds(r0, r1 - r0)],
                            dens_ref.at[pl.ds(q0, p1 - p0), pl.ds(t0, r1 - r0)],
                            halo_s.at[n], halo_r.at[n], b, d))
    for copy in to_core + to_x + to_z:
        copy.wait_send()
    for copy in halos:
        copy.wait()
    potential_from(dens_ref, out_ref, matrices, *fields)


def odd_of(v):
    return W3 * (v[0] + v[5]) + W25 * (v[1] + v[4]) + W150 * (v[2] + v[3])


def scaled_derivative(at):
    d = [at(o) - at(-o) for o in (1, 2, 3, 4)]
    return (D1 * d[0] + D2 * d[1]) + (D3 * d[2] - d[3])


def across_planes(ref, p, r0, rows):
    return scaled_derivative(lambda o: ref[p + o, pl.ds(r0, rows), :])


def across_rows(ref, p, r0, rows):
    return scaled_derivative(lambda o: ref[p, pl.ds(r0 + o, rows), :])


def dot(a, b):
    return jnp.dot(a, b, preferred_element_type=F32)


def potential_from(dens, out, matrices, f1, fe, fo, g3, ae, ao, be, bo, ce, co, le, lo):
    wide_w, low_w, deriv_w, weave_w = matrices

    def first(i, _):
        v = [dens[i + o] for o in range(6)]
        f1[2 * i] = v[2]
        f1[2 * i + 1] = odd_of(v)
        return 0
    lax.fori_loop(0, 12, first, 0)

    def second(p, _):
        v = [f1[p, pl.ds(2 + o, 24), :] for o in range(6)]
        fe[p, pl.ds(0, 24, stride=2), :] = v[2]
        fe[p, pl.ds(1, 24, stride=2), :] = odd_of(v)
        return 0
    lax.fori_loop(0, 24, second, 0)

    def split(p):
        high, low = two_terms(fe[pl.ds(p, 4)].reshape(192, 128))
        return high, jnp.concatenate([high, low], axis=1)

    def third_outer(p):
        _, both = split(p)
        fo[pl.ds(p, 4)] = dot(both, wide_w[:, 0:128]).reshape(4, 48, 128)

    def third_inner(i, _):
        p = 4 + 4 * i
        high, both = split(p)
        fo[pl.ds(p, 4)] = dot(both, wide_w[:, 0:128]).reshape(4, 48, 128)
        g = dot(both, wide_w[:, 128:384]) + dot(high, low_w[...])
        g3[0, pl.ds(4 * i, 4)] = g[:, 0:128].reshape(4, 48, 128)
        g3[1, pl.ds(4 * i, 4)] = g[:, 128:256].reshape(4, 48, 128)
        return 0
    third_outer(0)
    third_outer(20)
    lax.fori_loop(0, 4, third_inner, 0)

    def flux(p, r0, rows, inner):
        rs = pl.ds(r0, rows)
        for n, (src, a, b, c, local) in enumerate(((fe, ae, be, ce, le), (fo, ao, bo, co, lo))):
            f = src[p, rs, :]
            g1 = across_planes(src, p, r0, rows)
            g2 = across_rows(src, p, r0, rows)
            g_3 = g3[n, p - 4, rs, :]
            shifted = f * f + 0.01
            sixth = jnp.exp(jnp.log(shifted) * (1.0 / 6.0))
            t2 = sixth * sixth
            t4 = t2 * t2
            scaling = 0.01 * (t4 * t4)
            inverse = 1.0 / (scaling + (0.2195 / 0.804 / 78400.0) * (g1 * g1 + g2 * g2 + g_3 * g_3))
            share = scaling * inverse
            weight = ((0.2195 / 280.0) * share) * inverse
            a[p - 4, rs, :] = weight * g1
            if inner:
                b[p - 8, rs, :] = weight * g2
                c[p - 8, rs, :] = weight * g_3
                local[p - 8, rs, :] = sixth * (0.603 * share - 1.353)

    def outer(p, _):
        flux(p, 8, 32, False)
        return 0

    def inner(p, _):
        flux(p, 4, 40, True)
        return 0
    lax.fori_loop(4, 8, outer, 0)
    lax.fori_loop(8, 16, inner, 0)
    lax.fori_loop(16, 20, outer, 0)

    def last(i, _):
        p = 4 * i
        rows = pl.ds(8, 32)
        kept = ([], [], [], [])
        for n, (a, b, c, local) in enumerate(((ae, be, ce, le), (ao, bo, co, lo))):
            here = []
            for q in range(4):
                div = across_planes(a, p + q + 4, 8, 32) + across_rows(b, p + q, 8, 32)
                here.append(local[p + q, rows, :] + (0.2 / 280.0) * div)
            kept[0].append(jnp.concatenate(here, axis=0))
            kept[1].append(c[pl.ds(p, 4), rows, :].reshape(128, 128))
        res = []
        for values, w in ((kept[0], weave_w), (kept[1], deriv_w)):
            e, o = two_terms(values[0]), two_terms(values[1])
            res.append(dot(jnp.concatenate([e[0], o[0]], axis=1), w[...])
                       + dot(jnp.concatenate([e[1], o[1]], axis=1), w[...]))
        out[pl.ds(p, 4)] = (res[0] + (0.2 / 840.0) * res[1]).reshape(4, 32, 256)
        return 0
    lax.fori_loop(0, 2, last, 0)


def on_device(orbitals, occupations):
    dma = pltpu.SemaphoreType.DMA
    fine = pltpu.VMEM((24, 48, 128), F32)
    wide = pltpu.VMEM((16, 48, 128), F32)
    narrow = pltpu.VMEM((8, 48, 128), F32)
    return pl.pallas_call(
        kernel,
        out_shape=jax.ShapeDtypeStruct((8, 32, 256), F32),
        in_specs=[pl.BlockSpec(memory_space=pltpu.HBM), pl.BlockSpec(memory_space=pltpu.HBM)],
        out_specs=pl.BlockSpec(memory_space=pltpu.VMEM),
        scratch_shapes=[
            pltpu.SMEM((8,), F32), dma(()),
            pltpu.VMEM((17, 32, 128), F32),
            pltpu.VMEM((8, 8, 16, 16, 128), BF16),
            pltpu.VMEM((8, 2, 2, 4, 16, 128), F32),
            pltpu.VMEM((8, 2, 4, 16, 128), F32),
            pltpu.VMEM((8, 4, 16, 128), F32),
            pltpu.VMEM((7, 4, 16, 128), F32),
            dma((8,)), dma((8,)), dma((8,)), dma((8,)), dma((8,)), dma((7,)), dma((7,)),
            dma((len(PARTNERS),)), dma((len(PARTNERS),)),
            (pltpu.VMEM((256, 384), BF16), pltpu.VMEM((128, 256), BF16),
             pltpu.VMEM((256, 256), BF16), pltpu.VMEM((256, 256), BF16)),
            (pltpu.VMEM((24, 32, 128), F32), fine, fine, pltpu.VMEM((2, 16, 48, 128), F32), wide, wide,
             narrow, narrow, narrow, narrow, narrow, narrow),
        ],
        compiler_params=pltpu.CompilerParams(collective_id=0, has_side_effects=True,
                                             vmem_limit_bytes=53 * 1024 * 1024),
    )(pltpu.with_memory_space_constraint(occupations, pltpu.HBM), pltpu.with_memory_space_constraint(orbitals, pltpu.HBM))


def solution(mesh):
    return jax.shard_map(
        on_device,
        mesh=mesh,
        in_specs=(P("band", None, "dom", None), P("band")),
        out_specs=P("band", "dom", None),
        check_vma=False,
    )
```

```python
import jax
import jax.numpy as jnp
from jax import lax
from jax.experimental import pallas as pl
from jax.experimental.pallas import tpu as pltpu
from jax.sharding import PartitionSpec as P

MESH = pl.DeviceIdType.MESH
F32, BF16 = jnp.float32, jnp.bfloat16
W3, W25, W150 = 3.0 / 256.0, -25.0 / 256.0, 150.0 / 256.0
REFINE = {-2: W3, -1: W25, 0: W150, 1: W150, 2: W25, 3: W3}
D1, D2, D3, D4 = 224.0, -56.0, 32.0 / 3.0, -1.0
DERIV = {1: D1, 2: D2, 3: D3, 4: D4}

STEPS = (4, 3, 5, 1, 7, 2, 6, 0)
FAR = (4, 3, 5, 2, 6)
NEAR = (1, 7)
AROUND = tuple((j, e) for j in (1, -1, 0) for e in (1, -1, 0) if (j, e) != (0, 0))
PARTNERS = tuple((j, e) for j in (1, -1, 2, -2, 0) for e in (1, -1, 0) if (j, e) != (0, 0))


def fine_cell(r):
    if r % 2 == 0:
        return {r // 2: 1.0}
    return {(r - 1) // 2 + o: w for o, w in REFINE.items()}


def composed(r):
    out = {}
    for o, c in DERIV.items():
        for sign in (1, -1):
            for m, w in fine_cell(r + sign * o).items():
                out[m] = out.get(m, 0.0) + sign * c * w
    return out


def circulant(factors):
    source = lax.broadcasted_iota(jnp.int32, (128, 128), 0)
    target = lax.broadcasted_iota(jnp.int32, (128, 128), 1)
    offset = (source - target + 128) % 128
    out = jnp.zeros((128, 128), F32)
    for m, w in factors.items():
        out = jnp.where(offset == m % 128, w, out)
    return out


def two_terms(v):
    high = v.astype(BF16)
    return high, (v - high.astype(F32)).astype(BF16)


def build_matrices(wide_w, low_w, deriv_w, weave_w):
    refine = circulant(REFINE).astype(BF16)
    wide_w[0:128, 0:128] = refine
    wide_w[128:256, 0:128] = refine
    for r in (0, 1):
        high, low = two_terms(circulant(composed(r)))
        columns = slice(128 + 128 * r, 256 + 128 * r)
        wide_w[0:128, columns] = high
        wide_w[128:256, columns] = high
        low_w[:, 128 * r:128 * r + 128] = low
    for r in (0, 1):
        source = 2 * lax.broadcasted_iota(jnp.int32, (128, 256), 0) + r
        target = lax.broadcasted_iota(jnp.int32, (128, 256), 1)
        offset = (source - target + 256) % 256
        out = jnp.zeros((128, 256), F32)
        for o, c in ((1, 672.0), (2, -168.0), (3, 32.0), (4, -3.0)):
            out = jnp.where(offset == o, c, jnp.where(offset == 256 - o, -c, out))
        deriv_w[128 * r:128 * r + 128, :] = out.astype(BF16)
        weave_w[128 * r:128 * r + 128, :] = jnp.where(offset == 0, 1.0, 0.0).astype(BF16)


def kernel(occ_hbm, orb_ref, out_ref, occ_ref, occ_sem, dens_ref, orb, part, from_core, from_x, from_z, from_near,
           in_sem, core_s, core_r, x_s, x_r, z_s, z_r, near_s, near_r, near_ok, far_ok, halo_s, halo_r, matrices, fields):
    band = lax.axis_index("band")
    dom = lax.axis_index("dom")
    z, h, c = band // 4, (band // 2) % 2, band % 2
    other_c, other_h = 1 - c, 1 - h
    core_peer = z * 4 + h * 2 + other_c
    x_peer = z * 4 + other_h * 2 + c

    def z_peer(k):
        return (band + 4 * k) % 32

    def halo_peer(j, e):
        return (band + j + 32) % 32, (dom + e + 8) % 8

    def remote(src, dst, send_sem, recv_sem, b, d):
        copy = pltpu.make_async_remote_copy(
            src_ref=src, dst_ref=dst, send_sem=send_sem, recv_sem=recv_sem,
            device_id={"band": b, "dom": d}, device_id_type=MESH)
        copy.start()
        return copy

    occ_load = pltpu.make_async_copy(occ_hbm, occ_ref, occ_sem)
    occ_load.start()
    loads = []
    for s, k in enumerate(STEPS):
        first = ((z + k) % 8) * 16
        load = pltpu.make_async_copy(orb_ref.at[:, pl.ds(first, 16)], orb.at[s], in_sem.at[s])
        load.start()
        loads.append(load)

    barrier = pltpu.get_barrier_semaphore()

    def greet(b, d):
        pl.semaphore_signal(barrier, inc=1, device_id={"band": b, "dom": d}, device_id_type=MESH)

    greet(z * 4 + other_h * 2, dom)

    @pl.when(c == 1)
    def _():
        greet(z * 4 + h * 2, dom)

    for k in STEPS:
        if k:
            greet(z_peer(k) - c + 1, dom)
    for j, e in AROUND:
        greet((band - c + 1 + 2 * j + 32) % 32, (dom + e + 8) % 8)

    occ_load.wait()
    weights = [occ_ref[i] * (1.0 / 256.0) for i in range(8)]

    def band_sum(s):
        loads[s].wait()

        def planes(block, _):
            for p in range(4):
                total = jnp.zeros((16, 128), F32)
                for i in range(8):
                    value = orb[s, i, block * 4 + p].astype(F32)
                    total = total + weights[i] * (value * value)
                part[s, block % 2, block // 2, p] = total
            return 0

        lax.fori_loop(0, 4, planes, 0)

    to_core, to_x, to_z, to_near = [], {}, [], []

    def send_core(s):
        to_core.append(remote(part.at[s, other_c], from_core.at[s], core_s.at[s], core_r.at[s],
                              core_peer, dom))

    def send_x(s):
        to_core[s].wait_recv()
        from_core[s] = from_core[s] + part[s, c]
        if STEPS[s] in FAR:
            reduce_x(s)

    def reduce_x(s):
        to_x[s] = remote(from_core.at[s, other_h], from_x.at[s], x_s.at[s], x_r.at[s], x_peer, dom)

    def meet(sem, first_c, count):
        @pl.when(c == first_c)
        def _():
            pl.semaphore_wait(barrier, count)
            pl.semaphore_signal(sem, inc=1, device_id={"band": core_peer, "dom": dom}, device_id_type=MESH)

        @pl.when(c != first_c)
        def _():
            pl.semaphore_wait(sem, 1)

    for s in range(8):
        band_sum(s)
        if s == 0:
            meet(near_ok, 0, 3)
        send_core(s)
        if s >= 2:
            send_x(s - 2)
    send_x(6)
    send_x(7)
    meet(far_ok, 1, 2 * 7 + 2 * len(AROUND))
    for n, k in enumerate(NEAR):
        to_near.append(remote(from_core.at[STEPS.index(k)], from_near.at[n], near_s.at[n], near_r.at[n],
                              z_peer(k), dom))
    build_matrices(*matrices)
    for n, k in enumerate(FAR):
        if n == 2:
            for copy in to_near:
                copy.wait_recv()
            from_core[7] = from_core[7] + (from_near[0] + from_near[1])
            reduce_x(7)
        s = STEPS.index(k)
        to_x[s].wait_recv()
        from_x[s] = from_x[s] + from_core[s, h]
        to_z.append(remote(from_x.at[s], from_z.at[n], z_s.at[n], z_r.at[n], z_peer(k), dom))

    to_x[7].wait_recv()
    total = from_x[7] + from_core[7, h]
    for n in range(len(FAR)):
        to_z[n].wait_recv()
        total = total + from_z[n]
    dens_ref[6:10, 8:24, :] = total

    halos = []
    for n, (j, e) in enumerate(PARTNERS):
        p0, p1, q0 = {0: (0, 4, 6), 1: (0, 4, 2), -1: (0, 4, 10), 2: (2, 4, 0), -2: (0, 3, 14)}[j]
        r0, r1, t0 = {0: (8, 24, 8), 1: (16, 24, 0), -1: (8, 16, 24)}[e]
        b, d = halo_peer(j, e)
        halos.append(remote(dens_ref.at[pl.ds(6 + p0, p1 - p0), pl.ds(r0, r1 - r0)],
                            dens_ref.at[pl.ds(q0, p1 - p0), pl.ds(t0, r1 - r0)],
                            halo_s.at[n], halo_r.at[n], b, d))
    for copy in to_core + list(to_x.values()) + to_z + to_near:
        copy.wait_send()
    for copy in halos:
        copy.wait()
    potential_from(dens_ref, out_ref, matrices, *fields)


def odd_of(v):
    return W3 * (v[0] + v[5]) + W25 * (v[1] + v[4]) + W150 * (v[2] + v[3])


def scaled_derivative(at):
    d = [at(o) - at(-o) for o in (1, 2, 3, 4)]
    return (D1 * d[0] + D2 * d[1]) + (D3 * d[2] - d[3])


def across_planes(ref, p, r0, rows):
    return scaled_derivative(lambda o: ref[p + o, pl.ds(r0, rows), :])


def across_rows(ref, p, r0, rows):
    return scaled_derivative(lambda o: ref[p, pl.ds(r0 + o, rows), :])


def dot(a, b):
    return jnp.dot(a, b, preferred_element_type=F32)


def potential_from(dens, out, matrices, f1, fe, fo, g3, ae, ao, be, bo, ce, co, le, lo):
    wide_w, low_w, deriv_w, weave_w = matrices

    def first(i, _):
        v = [dens[i + o] for o in range(6)]
        f1[2 * i] = v[2]
        f1[2 * i + 1] = odd_of(v)
        return 0
    lax.fori_loop(0, 12, first, 0)

    def second(p, _):
        v = [f1[p, pl.ds(2 + o, 24), :] for o in range(6)]
        fe[p, pl.ds(0, 24, stride=2), :] = v[2]
        fe[p, pl.ds(1, 24, stride=2), :] = odd_of(v)
        return 0
    lax.fori_loop(0, 24, second, 0)

    def split(p):
        high, low = two_terms(fe[pl.ds(p, 4)].reshape(192, 128))
        return high, jnp.concatenate([high, low], axis=1)

    def third_outer(p):
        _, both = split(p)
        fo[pl.ds(p, 4)] = dot(both, wide_w[:, 0:128]).reshape(4, 48, 128)

    def third_inner(i, _):
        p = 4 + 4 * i
        high, both = split(p)
        fo[pl.ds(p, 4)] = dot(both, wide_w[:, 0:128]).reshape(4, 48, 128)
        g = dot(both, wide_w[:, 128:384]) + dot(high, low_w[...])
        g3[0, pl.ds(4 * i, 4)] = g[:, 0:128].reshape(4, 48, 128)
        g3[1, pl.ds(4 * i, 4)] = g[:, 128:256].reshape(4, 48, 128)
        return 0
    third_outer(0)
    third_outer(20)
    lax.fori_loop(0, 4, third_inner, 0)

    def flux(p, r0, rows, inner):
        rs = pl.ds(r0, rows)
        for n, (src, a, b, c, local) in enumerate(((fe, ae, be, ce, le), (fo, ao, bo, co, lo))):
            f = src[p, rs, :]
            g1 = across_planes(src, p, r0, rows)
            g2 = across_rows(src, p, r0, rows)
            g_3 = g3[n, p - 4, rs, :]
            shifted = f * f + 0.01
            sixth = jnp.exp(jnp.log(shifted) * (1.0 / 6.0))
            t2 = sixth * sixth
            t4 = t2 * t2
            scaling = 0.01 * (t4 * t4)
            inverse = 1.0 / (scaling + (0.2195 / 0.804 / 78400.0) * (g1 * g1 + g2 * g2 + g_3 * g_3))
            share = scaling * inverse
            weight = ((0.2195 / 280.0) * share) * inverse
            a[p - 4, rs, :] = weight * g1
            if inner:
                b[p - 8, rs, :] = weight * g2
                c[p - 8, rs, :] = weight * g_3
                local[p - 8, rs, :] = sixth * (0.603 * share - 1.353)

    def outer(p, _):
        flux(p, 8, 32, False)
        return 0

    def inner(p, _):
        flux(p, 4, 40, True)
        return 0
    lax.fori_loop(4, 8, outer, 0)
    lax.fori_loop(8, 16, inner, 0)
    lax.fori_loop(16, 20, outer, 0)

    def last(i, _):
        p = 4 * i
        rows = pl.ds(8, 32)
        kept = ([], [], [], [])
        for n, (a, b, c, local) in enumerate(((ae, be, ce, le), (ao, bo, co, lo))):
            here = []
            for q in range(4):
                div = across_planes(a, p + q + 4, 8, 32) + across_rows(b, p + q, 8, 32)
                here.append(local[p + q, rows, :] + (0.2 / 280.0) * div)
            kept[0].append(jnp.concatenate(here, axis=0))
            kept[1].append(c[pl.ds(p, 4), rows, :].reshape(128, 128))
        res = []
        for values, w in ((kept[0], weave_w), (kept[1], deriv_w)):
            e, o = two_terms(values[0]), two_terms(values[1])
            res.append(dot(jnp.concatenate([e[0], o[0]], axis=1), w[...])
                       + dot(jnp.concatenate([e[1], o[1]], axis=1), w[...]))
        out[pl.ds(p, 4)] = (res[0] + (0.2 / 840.0) * res[1]).reshape(4, 32, 256)
        return 0
    lax.fori_loop(0, 2, last, 0)


def on_device(orbitals, occupations):
    dma = pltpu.SemaphoreType.DMA
    fine = pltpu.VMEM((24, 48, 128), F32)
    wide = pltpu.VMEM((16, 48, 128), F32)
    narrow = pltpu.VMEM((8, 48, 128), F32)
    return pl.pallas_call(
        kernel,
        out_shape=jax.ShapeDtypeStruct((8, 32, 256), F32),
        in_specs=[pl.BlockSpec(memory_space=pltpu.HBM), pl.BlockSpec(memory_space=pltpu.HBM)],
        out_specs=pl.BlockSpec(memory_space=pltpu.VMEM),
        scratch_shapes=[
            pltpu.SMEM((8,), F32), dma(()),
            pltpu.VMEM((17, 32, 128), F32),
            pltpu.VMEM((8, 8, 16, 16, 128), BF16),
            pltpu.VMEM((8, 2, 2, 4, 16, 128), F32),
            pltpu.VMEM((8, 2, 4, 16, 128), F32),
            pltpu.VMEM((8, 4, 16, 128), F32),
            pltpu.VMEM((5, 4, 16, 128), F32),
            pltpu.VMEM((2, 2, 4, 16, 128), F32),
            dma((8,)), dma((8,)), dma((8,)), dma((8,)), dma((8,)), dma((5,)), dma((5,)),
            dma((2,)), dma((2,)), pltpu.SemaphoreType.REGULAR, pltpu.SemaphoreType.REGULAR,
            dma((len(PARTNERS),)), dma((len(PARTNERS),)),
            (pltpu.VMEM((256, 384), BF16), pltpu.VMEM((128, 256), BF16),
             pltpu.VMEM((256, 256), BF16), pltpu.VMEM((256, 256), BF16)),
            (pltpu.VMEM((24, 32, 128), F32), fine, fine, pltpu.VMEM((2, 16, 48, 128), F32), wide, wide,
             narrow, narrow, narrow, narrow, narrow, narrow),
        ],
        compiler_params=pltpu.CompilerParams(collective_id=0, has_side_effects=True,
                                             vmem_limit_bytes=53 * 1024 * 1024),
    )(pltpu.with_memory_space_constraint(occupations, pltpu.HBM), pltpu.with_memory_space_constraint(orbitals, pltpu.HBM))


def solution(mesh):
    return jax.shard_map(
        on_device,
        mesh=mesh,
        in_specs=(P("band", None, "dom", None), P("band")),
        out_specs=P("band", "dom", None),
        check_vma=False,
    )
```

```python
import math

import jax
import jax.numpy as jnp
from jax import lax
from jax.experimental import pallas as pl
from jax.experimental.pallas import tpu as pltpu
from jax.sharding import PartitionSpec as P

MESH = pl.DeviceIdType.MESH
F32, BF16 = jnp.float32, jnp.bfloat16
W3, W25, W150 = 3.0 / 256.0, -25.0 / 256.0, 150.0 / 256.0
REFINE = {-2: W3, -1: W25, 0: W150, 1: W150, 2: W25, 3: W3}
D1, D2, D3, D4 = 224.0, -56.0, 32.0 / 3.0, -1.0
DERIV = {1: D1, 2: D2, 3: D3, 4: D4}

STEPS = (4, 3, 5, 1, 7, 2, 6, 0)
FAR = (4, 3, 5, 2, 6)
NEAR = (1, 7)
LAG = 4
AROUND = tuple((j, e) for j in (1, -1, 0) for e in (1, -1, 0) if (j, e) != (0, 0))
PARTNERS = tuple((j, e) for j in (1, -1, 2, -2, 0) for e in (1, -1, 0) if (j, e) != (0, 0))


def fine_cell(r):
    if r % 2 == 0:
        return {r // 2: 1.0}
    return {(r - 1) // 2 + o: w for o, w in REFINE.items()}


def composed(r):
    out = {}
    for o, c in DERIV.items():
        for sign in (1, -1):
            for m, w in fine_cell(r + sign * o).items():
                out[m] = out.get(m, 0.0) + sign * c * w
    return out


def circulant(factors):
    source = lax.broadcasted_iota(jnp.int32, (128, 128), 0)
    target = lax.broadcasted_iota(jnp.int32, (128, 128), 1)
    offset = (source - target + 128) % 128
    out = jnp.zeros((128, 128), F32)
    for m, w in factors.items():
        out = jnp.where(offset == m % 128, w, out)
    return out


def two_terms(v):
    high = v.astype(BF16)
    return high, (v - high.astype(F32)).astype(BF16)


def build_matrices(wide_w, low_w, deriv_w, weave_w):
    refine = circulant(REFINE).astype(BF16)
    wide_w[0:128, 0:128] = refine
    wide_w[128:256, 0:128] = refine
    for r in (0, 1):
        high, low = two_terms(circulant(composed(r)))
        columns = slice(128 + 128 * r, 256 + 128 * r)
        wide_w[0:128, columns] = high
        wide_w[128:256, columns] = high
        low_w[:, 128 * r:128 * r + 128] = low
    for r in (0, 1):
        source = 2 * lax.broadcasted_iota(jnp.int32, (128, 256), 0) + r
        target = lax.broadcasted_iota(jnp.int32, (128, 256), 1)
        offset = (source - target + 256) % 256
        out = jnp.zeros((128, 256), F32)
        for o, c in ((1, 672.0), (2, -168.0), (3, 32.0), (4, -3.0)):
            out = jnp.where(offset == o, c, jnp.where(offset == 256 - o, -c, out))
        deriv_w[128 * r:128 * r + 128, :] = out.astype(BF16)
        weave_w[128 * r:128 * r + 128, :] = jnp.where(offset == 0, 1.0, 0.0).astype(BF16)


def kernel(occ_hbm, orb_ref, out_ref, occ_ref, occ_sem, dens_ref, orb, part, from_core, from_x, from_z, from_near,
           in_sem, core_s, core_r, x_s, x_r, z_s, z_r, near_s, near_r, near_ok, far_ok, halo_s, halo_r, matrices, fields):
    band = lax.axis_index("band")
    dom = lax.axis_index("dom")
    z, h, c = band // 4, (band // 2) % 2, band % 2
    other_c, other_h = 1 - c, 1 - h
    core_peer = z * 4 + h * 2 + other_c
    x_peer = z * 4 + other_h * 2 + c

    def z_peer(k):
        return (band + 4 * k) % 32

    def halo_peer(j, e):
        return (band + j + 32) % 32, (dom + e + 8) % 8

    def remote(src, dst, send_sem, recv_sem, b, d):
        copy = pltpu.make_async_remote_copy(
            src_ref=src, dst_ref=dst, send_sem=send_sem, recv_sem=recv_sem,
            device_id={"band": b, "dom": d}, device_id_type=MESH)
        copy.start()
        return copy

    occ_load = pltpu.make_async_copy(occ_hbm, occ_ref, occ_sem)
    occ_load.start()
    loads = []
    for s, k in enumerate(STEPS):
        first = ((z + k) % 8) * 16
        load = pltpu.make_async_copy(orb_ref.at[:, pl.ds(first, 16)], orb.at[s], in_sem.at[s])
        load.start()
        loads.append(load)

    barrier = pltpu.get_barrier_semaphore()

    def greet(b, d):
        pl.semaphore_signal(barrier, inc=1, device_id={"band": b, "dom": d}, device_id_type=MESH)

    greet(z * 4 + other_h * 2, dom)

    @pl.when(c == 1)
    def _():
        greet(z * 4 + h * 2, dom)

    for k in STEPS:
        if k:
            greet(z_peer(k) - c + 1, dom)
    for j, e in AROUND:
        greet((band - c + 1 + 2 * j + 32) % 32, (dom + e + 8) % 8)

    occ_load.wait()
    weights = [occ_ref[i] * (1.0 / 256.0) for i in range(8)]

    def band_sum(s):
        loads[s].wait()

        def planes(block, _):
            for p in range(4):
                total = jnp.zeros((16, 128), F32)
                for i in range(8):
                    value = orb[s, i, block * 4 + p].astype(F32)
                    total = total + weights[i] * (value * value)
                part[s, block % 2, block // 2, p] = total
            return 0

        lax.fori_loop(0, 4, planes, 0)

    to_core, to_x, to_z, to_near = [], {}, [], []

    def send_core(s):
        to_core.append(remote(part.at[s, other_c], from_core.at[s], core_s.at[s], core_r.at[s],
                              core_peer, dom))

    def send_x(s):
        to_core[s].wait_recv()
        from_core[s] = from_core[s] + part[s, c]
        if STEPS[s] in FAR:
            reduce_x(s)

    def reduce_x(s):
        to_x[s] = remote(from_core.at[s, other_h], from_x.at[s], x_s.at[s], x_r.at[s], x_peer, dom)

    def meet(sem, first_c, count):
        @pl.when(c == first_c)
        def _():
            pl.semaphore_wait(barrier, count)
            pl.semaphore_signal(sem, inc=1, device_id={"band": core_peer, "dom": dom}, device_id_type=MESH)

        @pl.when(c != first_c)
        def _():
            pl.semaphore_wait(sem, 1)

    for s in range(8):
        band_sum(s)
        if s == 0:
            meet(near_ok, 0, 3)
        send_core(s)
        if s >= LAG:
            send_x(s - LAG)
    for s in range(8 - LAG, 8):
        send_x(s)
    meet(far_ok, 1, 2 * 7 + 2 * len(AROUND))
    for n, k in enumerate(NEAR):
        to_near.append(remote(from_core.at[STEPS.index(k)], from_near.at[n], near_s.at[n], near_r.at[n],
                              z_peer(k), dom))
    build_matrices(*matrices)
    for n, k in enumerate(FAR):
        if n == 2:
            for copy in to_near:
                copy.wait_recv()
            from_core[7] = from_core[7] + (from_near[0] + from_near[1])
            reduce_x(7)
        s = STEPS.index(k)
        to_x[s].wait_recv()
        from_x[s] = from_x[s] + from_core[s, h]
        to_z.append(remote(from_x.at[s], from_z.at[n], z_s.at[n], z_r.at[n], z_peer(k), dom))

    to_x[7].wait_recv()
    total = from_x[7] + from_core[7, h]
    for n in range(len(FAR)):
        to_z[n].wait_recv()
        total = total + from_z[n]
    dens_ref[6:10, 8:24, :] = total

    halos = []
    for n, (j, e) in enumerate(PARTNERS):
        p0, p1, q0 = {0: (0, 4, 6), 1: (0, 4, 2), -1: (0, 4, 10), 2: (2, 4, 0), -2: (0, 3, 14)}[j]
        r0, r1, t0 = {0: (8, 24, 8), 1: (18, 24, 2), -1: (8, 15, 24)}[e]
        b, d = halo_peer(j, e)
        halos.append(remote(dens_ref.at[pl.ds(6 + p0, p1 - p0), pl.ds(r0, r1 - r0)],
                            dens_ref.at[pl.ds(q0, p1 - p0), pl.ds(t0, r1 - r0)],
                            halo_s.at[n], halo_r.at[n], b, d))
    def own_rows_here():
        for copy, (_, e) in zip(halos, PARTNERS):
            if e == 0:
                copy.wait_recv()

    def all_here():
        for copy, (_, e) in zip(halos, PARTNERS):
            if e != 0:
                copy.wait_recv()

    potential_from(own_rows_here, all_here, dens_ref, out_ref, matrices, *fields)
    for copy in to_core + list(to_x.values()) + to_z + to_near + halos:
        copy.wait_send()


def odd_of(v):
    return W3 * (v[0] + v[5]) + W25 * (v[1] + v[4]) + W150 * (v[2] + v[3])


def scaled_derivative(at):
    d = [at(o) - at(-o) for o in (1, 2, 3, 4)]
    return (D1 * d[0] + D2 * d[1]) + (D3 * d[2] - d[3])


def across_planes(ref, p, r0, rows):
    return scaled_derivative(lambda o: ref[p + o, pl.ds(r0, rows), :])


def across_rows(ref, p, r0, rows):
    return scaled_derivative(lambda o: ref[p, pl.ds(r0 + o, rows), :])


def dot(a, b):
    return jnp.dot(a, b, preferred_element_type=F32)


def potential_from(own_rows_here, all_here, dens, out, matrices, f1, fe, fo, g3, ae, ao, be, bo, ce, co, le, lo, rest, turn):
    wide_w, low_w, deriv_w, weave_w = matrices

    def first(*groups):
        def body(i, _):
            for r0, rows in groups:
                rs = pl.ds(r0, rows)
                v = [dens[i + o, rs, :] for o in range(6)]
                f1[2 * i, rs, :] = v[2]
                f1[2 * i + 1, rs, :] = odd_of(v)
            return 0
        lax.fori_loop(0, 12, body, 0)

    def second(*starts):
        def body(i, _):
            for p in (2 * i, 2 * i + 1):
                for r0 in starts:
                    v = [f1[p, pl.ds(r0 // 2 + 2 + o, 8), :] for o in range(6)]
                    fe[p, pl.ds(r0, 8, stride=2), :] = v[2]
                    fe[p, pl.ds(r0 + 1, 8, stride=2), :] = odd_of(v)
            return 0
        lax.fori_loop(0, 12, body, 0)

    def third(*starts):
        cells = jnp.concatenate([fe[:, pl.ds(r0, 16), :].reshape(384, 128) for r0 in starts], axis=0)
        high, low = two_terms(cells)
        both = jnp.concatenate([high, low], axis=1)
        odd = dot(both, wide_w[:, 0:128])

        def inner(v):
            return jnp.concatenate([v[384 * i + 64:384 * i + 320] for i in range(len(starts))], axis=0)

        g = dot(inner(both), wide_w[:, 128:384]) + dot(inner(high), low_w[...])
        for i, r0 in enumerate(starts):
            rs = pl.ds(r0, 16)
            fo[:, rs, :] = odd[384 * i:384 * i + 384].reshape(24, 16, 128)
            for r in (0, 1):
                g3[r, :, rs, :] = g[256 * i:256 * i + 256, 128 * r:128 * r + 128].reshape(16, 16, 128)

    def flux_of(p, r0, rows, inner):
        rs = pl.ds(r0, rows)
        for n, (src, a, b, c, local) in enumerate(((fe, ae, be, ce, le), (fo, ao, bo, co, lo))):
            f = src[p, rs, :]
            g1 = across_planes(src, p, r0, rows)
            g2 = across_rows(src, p, r0, rows)
            g_3 = g3[n, p - 4, rs, :]
            shifted = f * f + 0.01
            sixth = jnp.exp2(jnp.log(shifted) * (1.0 / (6.0 * math.log(2.0))))
            t2 = sixth * sixth
            t4 = t2 * t2
            scaling = 0.01 * (t4 * t4)
            inverse = 1.0 / (scaling + (0.2195 / 0.804 / 78400.0) * (g1 * g1 + g2 * g2 + g_3 * g_3))
            share = scaling * inverse
            weight = ((0.2195 / 280.0) * share) * inverse
            a[p - 4, rs, :] = weight * g1
            if inner:
                b[p - 8, rs, :] = weight * g2
                c[p - 8, rs, :] = weight * g_3
                local[p - 8, rs, :] = sixth * (0.603 * share - 1.353)

    def flux(step, *groups):
        for lo_p, hi_p, inner in ((4, 8, False), (8, 16, True), (16, 20, False)):
            def body(i, _):
                for q in range(step):
                    for r0, rows in groups:
                        flux_of(lo_p + i * step + q, r0, rows, inner)
                return 0
            lax.fori_loop(0, (hi_p - lo_p) // step, body, 0)

    own_rows_here()
    first((8, 16))
    second(16)
    third(16)
    flux(2, (20, 8))
    all_here()
    first((0, 8), (24, 8))
    second(0, 32)
    third(0, 32)
    flux(2, (4, 16), (28, 16))

    def last(p, _):
        rows = pl.ds(8, 32)
        for n, (a, b, c, local) in enumerate(((ae, be, ce, le), (ao, bo, co, lo))):
            lanes = slice(128 * n, 128 * n + 128)
            div = across_planes(a, p + 4, 8, 32) + across_rows(b, p, 8, 32)
            for ref, value in ((rest, local[p, rows, :] + (0.2 / 280.0) * div), (turn, c[p, rows, :])):
                high, low = two_terms(value)
                ref[pl.ds(pl.multiple_of(32 * p, 32), 32), lanes] = high
                ref[pl.ds(pl.multiple_of(32 * p + 256, 32), 32), lanes] = low
        return 0
    lax.fori_loop(0, 8, last, 0)
    woven, derived = dot(rest[...], weave_w[...]), dot(turn[...], deriv_w[...])
    out[...] = ((woven[:256] + woven[256:]) + (0.2 / 840.0) * (derived[:256] + derived[256:])).reshape(8, 32, 256)


def on_device(orbitals, occupations):
    dma = pltpu.SemaphoreType.DMA
    fine = pltpu.VMEM((24, 48, 128), F32)
    wide = pltpu.VMEM((16, 48, 128), F32)
    narrow = pltpu.VMEM((8, 48, 128), F32)
    return pl.pallas_call(
        kernel,
        out_shape=jax.ShapeDtypeStruct((8, 32, 256), F32),
        in_specs=[pl.BlockSpec(memory_space=pltpu.HBM), pl.BlockSpec(memory_space=pltpu.HBM)],
        out_specs=pl.BlockSpec(memory_space=pltpu.VMEM),
        scratch_shapes=[
            pltpu.SMEM((8,), F32), dma(()),
            pltpu.VMEM((17, 32, 128), F32),
            pltpu.VMEM((8, 8, 16, 16, 128), BF16),
            pltpu.VMEM((8, 2, 2, 4, 16, 128), F32),
            pltpu.VMEM((8, 2, 4, 16, 128), F32),
            pltpu.VMEM((8, 4, 16, 128), F32),
            pltpu.VMEM((5, 4, 16, 128), F32),
            pltpu.VMEM((2, 2, 4, 16, 128), F32),
            dma((8,)), dma((8,)), dma((8,)), dma((8,)), dma((8,)), dma((5,)), dma((5,)),
            dma((2,)), dma((2,)), pltpu.SemaphoreType.REGULAR, pltpu.SemaphoreType.REGULAR,
            dma((len(PARTNERS),)), dma((len(PARTNERS),)),
            (pltpu.VMEM((256, 384), BF16), pltpu.VMEM((128, 256), BF16),
             pltpu.VMEM((256, 256), BF16), pltpu.VMEM((256, 256), BF16)),
            (pltpu.VMEM((24, 32, 128), F32), fine, fine, pltpu.VMEM((2, 16, 48, 128), F32), wide, wide,
             narrow, narrow, narrow, narrow, narrow, narrow, pltpu.VMEM((512, 256), BF16), pltpu.VMEM((512, 256), BF16)),
        ],
        compiler_params=pltpu.CompilerParams(collective_id=0, has_side_effects=True,
                                             vmem_limit_bytes=53 * 1024 * 1024),
    )(pltpu.with_memory_space_constraint(occupations, pltpu.HBM), pltpu.with_memory_space_constraint(orbitals, pltpu.HBM))


def solution(mesh):
    return jax.shard_map(
        on_device,
        mesh=mesh,
        in_specs=(P("band", None, "dom", None), P("band")),
        out_specs=P("band", "dom", None),
        check_vma=False,
    )
```

```python
import math

import jax
import jax.numpy as jnp
from jax import lax
from jax.experimental import pallas as pl
from jax.experimental.pallas import tpu as pltpu
from jax.sharding import PartitionSpec as P

MESH = pl.DeviceIdType.MESH
F32, BF16 = jnp.float32, jnp.bfloat16
W3, W25, W150 = 3.0 / 256.0, -25.0 / 256.0, 150.0 / 256.0
REFINE = {-2: W3, -1: W25, 0: W150, 1: W150, 2: W25, 3: W3}
D1, D2, D3, D4 = 224.0, -56.0, 32.0 / 3.0, -1.0
DERIV = {1: D1, 2: D2, 3: D3, 4: D4}

STEPS = (4, 3, 2, 1, 5, 6, 7, 0)
FAR = (4, 3, 2, 5, 6)
NEAR = (1, 7)
LAG = 4
AROUND = tuple((j, e) for j in (1, -1, 0) for e in (1, -1, 0) if (j, e) != (0, 0))
PARTNERS = tuple((j, e) for j in (1, -1, 2, -2, 0) for e in (1, -1, 0) if (j, e) != (0, 0))


def fine_cell(r):
    if r % 2 == 0:
        return {r // 2: 1.0}
    return {(r - 1) // 2 + o: w for o, w in REFINE.items()}


def composed(r):
    out = {}
    for o, c in DERIV.items():
        for sign in (1, -1):
            for m, w in fine_cell(r + sign * o).items():
                out[m] = out.get(m, 0.0) + sign * c * w
    return out


def circulant(factors):
    source = lax.broadcasted_iota(jnp.int32, (128, 128), 0)
    target = lax.broadcasted_iota(jnp.int32, (128, 128), 1)
    offset = (source - target + 128) % 128
    out = jnp.zeros((128, 128), F32)
    for m, w in factors.items():
        out = jnp.where(offset == m % 128, w, out)
    return out


def two_terms(v):
    high = v.astype(BF16)
    return high, (v - high.astype(F32)).astype(BF16)


def build_matrices(wide_w, low_w, deriv_w, weave_w):
    refine = circulant(REFINE).astype(BF16)
    for t in (0, 128, 256):
        wide_w[t:t + 128, 0:128] = refine
    for r in (0, 1):
        high, low = two_terms(circulant(composed(r)))
        columns = slice(128 + 128 * r, 256 + 128 * r)
        for t in (0, 128, 256):
            wide_w[t:t + 128, columns] = high
        for t in (0, 128):
            low_w[t:t + 128, 128 * r:128 * r + 128] = low
    for r in (0, 1):
        source = 2 * lax.broadcasted_iota(jnp.int32, (128, 256), 0) + r
        target = lax.broadcasted_iota(jnp.int32, (128, 256), 1)
        offset = (source - target + 256) % 256
        out = jnp.zeros((128, 256), F32)
        for o, c in ((1, 672.0), (2, -168.0), (3, 32.0), (4, -3.0)):
            out = jnp.where(offset == o, c, jnp.where(offset == 256 - o, -c, out))
        deriv_w[128 * r:128 * r + 128, :] = out.astype(BF16)
        weave_w[128 * r:128 * r + 128, :] = jnp.where(offset == 0, 1.0, 0.0).astype(BF16)


def kernel(occ_hbm, orb_ref, out_ref, occ_ref, occ_sem, dens_ref, orb, part, from_core, from_x, from_z, from_near,
           in_sem, core_s, core_r, x_s, x_r, z_s, z_r, near_s, near_r, near_ok, far_ok, halo_s, halo_r, matrices, fields):
    band = lax.axis_index("band")
    dom = lax.axis_index("dom")
    z, h, c = band // 4, (band // 2) % 2, band % 2
    other_c, other_h = 1 - c, 1 - h
    core_peer = z * 4 + h * 2 + other_c
    x_peer = z * 4 + other_h * 2 + c

    def z_peer(k):
        return (band + 4 * k) % 32

    def halo_peer(j, e):
        return (band + j + 32) % 32, (dom + e + 8) % 8

    def remote(src, dst, send_sem, recv_sem, b, d):
        copy = pltpu.make_async_remote_copy(
            src_ref=src, dst_ref=dst, send_sem=send_sem, recv_sem=recv_sem,
            device_id={"band": b, "dom": d}, device_id_type=MESH)
        copy.start()
        return copy

    occ_load = pltpu.make_async_copy(occ_hbm, occ_ref, occ_sem)
    occ_load.start()
    loads = []
    for s, k in enumerate(STEPS):
        first = ((z + k) % 8) * 16
        load = pltpu.make_async_copy(orb_ref.at[:, pl.ds(first, 16)], orb.at[s], in_sem.at[s])
        load.start()
        loads.append(load)

    barrier = pltpu.get_barrier_semaphore()

    def greet(b, d):
        pl.semaphore_signal(barrier, inc=1, device_id={"band": b, "dom": d}, device_id_type=MESH)

    greet(z * 4 + other_h * 2, dom)

    @pl.when(c == 1)
    def _():
        greet(z * 4 + h * 2, dom)

    for k in STEPS:
        if k:
            greet(z_peer(k) - c + 1, dom)
    for j, e in AROUND:
        greet((band - c + 1 + 2 * j + 32) % 32, (dom + e + 8) % 8)

    occ_load.wait()
    weights = [occ_ref[i] * (1.0 / 256.0) for i in range(8)]

    def band_sum(s):
        loads[s].wait()

        def planes(block, _):
            for p in range(4):
                total = jnp.zeros((16, 128), F32)
                for i in range(8):
                    value = orb[s, i, block * 4 + p].astype(F32)
                    total = total + weights[i] * (value * value)
                part[s, block % 2, block // 2, p] = total
            return 0

        lax.fori_loop(0, 4, planes, 0)

    to_core, to_x, to_z, to_near = [], {}, [], []

    def send_core(s):
        to_core.append(remote(part.at[s, other_c], from_core.at[s], core_s.at[s], core_r.at[s],
                              core_peer, dom))

    def send_x(s):
        to_core[s].wait_recv()
        from_core[s] = from_core[s] + part[s, c]
        if STEPS[s] in FAR:
            reduce_x(s)

    def reduce_x(s):
        to_x[s] = remote(from_core.at[s, other_h], from_x.at[s], x_s.at[s], x_r.at[s], x_peer, dom)

    def meet(sem, first_c, count):
        @pl.when(c == first_c)
        def _():
            pl.semaphore_wait(barrier, count)
            pl.semaphore_signal(sem, inc=1, device_id={"band": core_peer, "dom": dom}, device_id_type=MESH)

        @pl.when(c != first_c)
        def _():
            pl.semaphore_wait(sem, 1)

    for s in range(8):
        band_sum(s)
        if s == 0:
            meet(near_ok, 0, 3)
        send_core(s)
        if s >= LAG:
            send_x(s - LAG)
    for s in range(8 - LAG, 8):
        send_x(s)
    meet(far_ok, 1, 2 * 7 + 2 * len(AROUND))
    for n, k in enumerate(NEAR):
        to_near.append(remote(from_core.at[STEPS.index(k)], from_near.at[n], near_s.at[n], near_r.at[n],
                              z_peer(k), dom))
    build_matrices(*matrices)
    for n, k in enumerate(FAR):
        if n == 3:
            for copy in to_near:
                copy.wait_recv()
            from_core[7] = from_core[7] + (from_near[0] + from_near[1])
            reduce_x(7)
        s = STEPS.index(k)
        to_x[s].wait_recv()
        from_x[s] = from_x[s] + from_core[s, h]
        to_z.append(remote(from_x.at[s], from_z.at[n], z_s.at[n], z_r.at[n], z_peer(k), dom))

    to_x[7].wait_recv()
    total = from_x[7] + from_core[7, h]
    for n in range(len(FAR)):
        to_z[n].wait_recv()
        total = total + from_z[n]
    dens_ref[6:10, 8:24, :] = total

    halos = []
    for n, (j, e) in enumerate(PARTNERS):
        p0, p1, q0 = {0: (0, 4, 6), 1: (0, 4, 2), -1: (0, 4, 10), 2: (2, 4, 0), -2: (0, 3, 14)}[j]
        r0, r1, t0 = {0: (8, 24, 8), 1: (18, 24, 2), -1: (8, 15, 24)}[e]
        b, d = halo_peer(j, e)
        halos.append(remote(dens_ref.at[pl.ds(6 + p0, p1 - p0), pl.ds(r0, r1 - r0)],
                            dens_ref.at[pl.ds(q0, p1 - p0), pl.ds(t0, r1 - r0)],
                            halo_s.at[n], halo_r.at[n], b, d))
    def own_rows_here():
        for copy, (_, e) in zip(halos, PARTNERS):
            if e == 0:
                copy.wait_recv()

    def all_here():
        for copy, (_, e) in zip(halos, PARTNERS):
            if e != 0:
                copy.wait_recv()

    potential_from(own_rows_here, all_here, dens_ref, out_ref, matrices, *fields)
    for copy in to_core + list(to_x.values()) + to_z + to_near + halos:
        copy.wait_send()


def odd_of(v):
    return W3 * (v[0] + v[5]) + W25 * (v[1] + v[4]) + W150 * (v[2] + v[3])


def scaled_derivative(at):
    d = [at(o) - at(-o) for o in (1, 2, 3, 4)]
    return (D1 * d[0] + D2 * d[1]) + (D3 * d[2] - d[3])


def across_planes(ref, p, r0, rows):
    return scaled_derivative(lambda o: ref[p + o, pl.ds(r0, rows), :])


def across_rows(ref, p, r0, rows):
    return scaled_derivative(lambda o: ref[p, pl.ds(r0 + o, rows), :])


def dot(a, b):
    return jnp.dot(a, b, preferred_element_type=F32)


def potential_from(own_rows_here, all_here, dens, out, matrices, f1, fe, fo, g3, ae, ao, be, bo, ce, co, le, lo, rest, turn):
    wide_w, low_w, deriv_w, weave_w = matrices

    def first(*groups):
        def body(i, _):
            for r0, rows in groups:
                rs = pl.ds(r0, rows)
                v = [dens[i + o, rs, :] for o in range(6)]
                f1[2 * i, rs, :] = v[2]
                f1[2 * i + 1, rs, :] = odd_of(v)
            return 0
        lax.fori_loop(0, 12, body, 0)

    def second(*starts):
        def body(i, _):
            for p in (2 * i, 2 * i + 1):
                for r0 in starts:
                    v = [f1[p, pl.ds(r0 // 2 + 2 + o, 8), :] for o in range(6)]
                    fe[p, pl.ds(r0, 8, stride=2), :] = v[2]
                    fe[p, pl.ds(r0 + 1, 8, stride=2), :] = odd_of(v)
            return 0
        lax.fori_loop(0, 12, body, 0)

    def third(*starts):
        cells = jnp.concatenate([fe[:, pl.ds(r0, 16), :].reshape(384, 128) for r0 in starts], axis=0)
        high = cells.astype(BF16)
        middle, low = two_terms(cells - high.astype(F32))
        terms = jnp.concatenate([high, middle, low], axis=1)
        odd = dot(terms, wide_w[:, 0:128])

        def inner(v):
            return jnp.concatenate([v[384 * i + 64:384 * i + 320] for i in range(len(starts))], axis=0)

        kept = inner(terms)
        g = dot(kept, wide_w[:, 128:384]) + dot(kept[:, 0:256], low_w[...])
        for i, r0 in enumerate(starts):
            rs = pl.ds(r0, 16)
            fo[:, rs, :] = odd[384 * i:384 * i + 384].reshape(24, 16, 128)
            for r in (0, 1):
                g3[r, :, rs, :] = g[256 * i:256 * i + 256, 128 * r:128 * r + 128].reshape(16, 16, 128)

    def flux_of(p, r0, rows, inner):
        rs = pl.ds(r0, rows)
        for n, (src, a, b, c, local) in enumerate(((fe, ae, be, ce, le), (fo, ao, bo, co, lo))):
            f = src[p, rs, :]
            g1 = across_planes(src, p, r0, rows)
            g2 = across_rows(src, p, r0, rows)
            g_3 = g3[n, p - 4, rs, :]
            shifted = f * f + 0.01
            sixth = jnp.exp2(jnp.log(shifted) * (1.0 / (6.0 * math.log(2.0))))
            t2 = sixth * sixth
            t4 = t2 * t2
            scaling = 0.01 * (t4 * t4)
            inverse = 1.0 / (scaling + (0.2195 / 0.804 / 78400.0) * (g1 * g1 + g2 * g2 + g_3 * g_3))
            share = scaling * inverse
            weight = ((0.2195 / 280.0) * share) * inverse
            a[p - 4, rs, :] = weight * g1
            if inner:
                b[p - 8, rs, :] = weight * g2
                c[p - 8, rs, :] = weight * g_3
                local[p - 8, rs, :] = sixth * (0.603 * share - 1.353)

    def flux(step, *groups):
        for lo_p, hi_p, inner in ((4, 8, False), (8, 16, True), (16, 20, False)):
            def body(i, _):
                for q in range(step):
                    for r0, rows in groups:
                        flux_of(lo_p + i * step + q, r0, rows, inner)
                return 0
            lax.fori_loop(0, (hi_p - lo_p) // step, body, 0)

    own_rows_here()
    first((8, 16))
    second(16)
    third(16)
    flux(2, (20, 8))
    all_here()
    first((0, 8), (24, 8))
    second(0, 32)
    third(0, 32)
    flux(2, (4, 16), (28, 16))

    def last(p, _):
        rows = pl.ds(8, 32)
        for n, (a, b, c, local) in enumerate(((ae, be, ce, le), (ao, bo, co, lo))):
            lanes = slice(128 * n, 128 * n + 128)
            div = across_planes(a, p + 4, 8, 32) + across_rows(b, p, 8, 32)
            for ref, value in ((rest, local[p, rows, :] + (0.2 / 280.0) * div), (turn, c[p, rows, :])):
                high, low = two_terms(value)
                ref[pl.ds(pl.multiple_of(32 * p, 32), 32), lanes] = high
                ref[pl.ds(pl.multiple_of(32 * p + 256, 32), 32), lanes] = low
        return 0
    lax.fori_loop(0, 8, last, 0)
    woven, derived = dot(rest[...], weave_w[...]), dot(turn[...], deriv_w[...])
    out[...] = ((woven[:256] + woven[256:]) + (0.2 / 840.0) * (derived[:256] + derived[256:])).reshape(8, 32, 256)


def on_device(orbitals, occupations):
    dma = pltpu.SemaphoreType.DMA
    fine = pltpu.VMEM((24, 48, 128), F32)
    wide = pltpu.VMEM((16, 48, 128), F32)
    narrow = pltpu.VMEM((8, 48, 128), F32)
    return pl.pallas_call(
        kernel,
        out_shape=jax.ShapeDtypeStruct((8, 32, 256), F32),
        in_specs=[pl.BlockSpec(memory_space=pltpu.HBM), pl.BlockSpec(memory_space=pltpu.HBM)],
        out_specs=pl.BlockSpec(memory_space=pltpu.VMEM),
        scratch_shapes=[
            pltpu.SMEM((8,), F32), dma(()),
            pltpu.VMEM((17, 32, 128), F32),
            pltpu.VMEM((8, 8, 16, 16, 128), BF16),
            pltpu.VMEM((8, 2, 2, 4, 16, 128), F32),
            pltpu.VMEM((8, 2, 4, 16, 128), F32),
            pltpu.VMEM((8, 4, 16, 128), F32),
            pltpu.VMEM((5, 4, 16, 128), F32),
            pltpu.VMEM((2, 2, 4, 16, 128), F32),
            dma((8,)), dma((8,)), dma((8,)), dma((8,)), dma((8,)), dma((5,)), dma((5,)),
            dma((2,)), dma((2,)), pltpu.SemaphoreType.REGULAR, pltpu.SemaphoreType.REGULAR,
            dma((len(PARTNERS),)), dma((len(PARTNERS),)),
            (pltpu.VMEM((384, 384), BF16), pltpu.VMEM((256, 256), BF16),
             pltpu.VMEM((256, 256), BF16), pltpu.VMEM((256, 256), BF16)),
            (pltpu.VMEM((24, 32, 128), F32), fine, fine, pltpu.VMEM((2, 16, 48, 128), F32), wide, wide,
             narrow, narrow, narrow, narrow, narrow, narrow, pltpu.VMEM((512, 256), BF16), pltpu.VMEM((512, 256), BF16)),
        ],
        compiler_params=pltpu.CompilerParams(collective_id=0, has_side_effects=True,
                                             vmem_limit_bytes=53 * 1024 * 1024),
    )(pltpu.with_memory_space_constraint(occupations, pltpu.HBM), pltpu.with_memory_space_constraint(orbitals, pltpu.HBM))


def solution(mesh):
    return jax.shard_map(
        on_device,
        mesh=mesh,
        in_specs=(P("band", None, "dom", None), P("band")),
        out_specs=P("band", "dom", None),
        check_vma=False,
    )
```
